64 devices in a mesh: replica: 4 (over x, y), data: 16 (over z, core).
Axes of the slice: x: 2, y: 2, z: 8, core: 2. Of those that a mesh axis runs over, the one named last changes fastest.
The devices are a block of a 4x4x8 slice.
Arguments:
- q_hidden: bfloat16 [512, 20, 1536], P(('replica', 'data')), parts along dimension 0
- d_hidden: bfloat16 [512, 768, 1536], P(('replica', 'data')), parts along dimension 0
- w_proj: bfloat16 [1536, 128], replicated
- q_mask: int32 [512, 20], P(('replica', 'data')), parts along dimension 0
- d_mask: int32 [512, 768], P(('replica', 'data')), parts along dimension 0
- temperature: float32 [], replicated
Outputs:
- output 1: float32 [512], P(('replica', 'data')), parts along dimension 0
- output 2: float32 [512], P(('replica', 'data')), parts along dimension 0
- output 3: float32 [4], P('replica'), parts along dimension 0
There are 4 independent parts. The reference program is written for one: setup_inputs(seed, part) draws one part's arguments, and reference() takes and returns one part's arrays. A program takes and returns all parts, laid end to end along the dimension named above; an argument that names none is the same for every part.
All inputs are finite; a program needn't handle non-finite values.
Results may differ from the reference program's by a relative error of at most 0.001.
Values are sent between devices in bfloat16 or wider.
A program may use at most 768 MiB of HBM per device.

```python
import jax
import jax.numpy as jnp
from jax import lax

HIDDEN = 1536
PROJ_DIM = 128
Q_LEN = 20
DOC_LEN = 768
GROUP_PAIRS = 128


def setup_inputs(seed: int = 0, part: int = 0) -> dict:
    root_key = jax.random.key(seed)
    shared_keys = jax.random.split(jax.random.fold_in(root_key, 1), 2)
    part_keys = jax.random.split(jax.random.fold_in(jax.random.fold_in(root_key, 2), part), 6)
    w_proj = jax.random.normal(shared_keys[0], (HIDDEN, PROJ_DIM), jnp.float32) * HIDDEN ** -0.5
    temperature = jax.random.uniform(shared_keys[1], (), jnp.float32, 0.12, 0.2) * Q_LEN
    common = jax.random.normal(part_keys[0], (HIDDEN,), jnp.float32)
    topics = jax.random.normal(part_keys[1], (GROUP_PAIRS, HIDDEN), jnp.float32)
    q_noise = jax.random.normal(part_keys[2], (GROUP_PAIRS, Q_LEN, HIDDEN), jnp.float32)
    d_noise = jax.random.normal(part_keys[3], (GROUP_PAIRS, DOC_LEN, HIDDEN), jnp.float32)
    q_lens = jax.random.randint(part_keys[4], (GROUP_PAIRS,), Q_LEN // 2, Q_LEN + 1)
    d_lens = jax.random.randint(part_keys[5], (GROUP_PAIRS,), DOC_LEN // 4, DOC_LEN + 1)
    q_mask = (jnp.arange(Q_LEN)[None, :] < q_lens[:, None]).astype(jnp.int32)
    d_mask = (jnp.arange(DOC_LEN)[None, :] < d_lens[:, None]).astype(jnp.int32)
    q_real = common + topics[:, None, :] + q_noise
    q_pad = common + 2.0 * jnp.roll(topics, 1, axis=0)[:, None, :] + 0.5 * q_noise
    d_real = common + topics[:, None, :] + d_noise
    d_pad = 4.0 * common + 0.5 * d_noise
    q_hidden = jnp.where(q_mask[:, :, None] == 1, q_real, q_pad).astype(jnp.bfloat16)
    d_hidden = jnp.where(d_mask[:, :, None] == 1, d_real, d_pad).astype(jnp.bfloat16)
    return {'q_hidden': q_hidden, 'd_hidden': d_hidden, 'w_proj': w_proj.astype(jnp.bfloat16), 'q_mask': q_mask, 'd_mask': d_mask, 'temperature': temperature}


def project(hidden, w_proj):
    flat_rows = hidden.reshape(-1, hidden.shape[-1])
    raw_proj = jnp.dot(flat_rows, w_proj, preferred_element_type=jnp.float32)
    unit_vecs = raw_proj / jnp.sqrt(jnp.sum(raw_proj * raw_proj, axis=-1, keepdims=True))
    return unit_vecs.astype(jnp.bfloat16).reshape(hidden.shape[:-1] + (w_proj.shape[1],))


def reference(q_hidden, d_hidden, w_proj, q_mask, d_mask, temperature):
    q_vecs = project(q_hidden, w_proj).astype(jnp.float32)
    p_vecs = project(d_hidden, w_proj).astype(jnp.float32)
    doc_valid = d_mask == 1

    def score_row(row_args):
        q_row, q_valid = row_args
        sim_vals = jnp.einsum('tk,jsk->tjs', q_row, p_vecs)
        best_sim = jnp.max(jnp.where(doc_valid[None, :, :], sim_vals, -jnp.inf), axis=2)
        return jnp.sum(jnp.where(q_valid[:, None] == 1, best_sim, 0.0), axis=0)

    scores = lax.map(score_row, (q_vecs, q_mask))
    logits = scores / temperature
    pos_logit = jnp.diagonal(logits)
    loss_query = jax.nn.logsumexp(logits, axis=1) - pos_logit
    loss_doc = jax.nn.logsumexp(logits, axis=0) - pos_logit
    loss_mean = (0.5 * jnp.mean(loss_query + loss_doc)).reshape(1)
    return loss_query, loss_doc, loss_mean
```

```python
import functools

import jax
import jax.numpy as jnp
from jax import lax
from jax.experimental import pallas as pl
from jax.experimental.pallas import tpu as pltpu
from jax.sharding import PartitionSpec as P

MESH = pl.DeviceIdType.MESH
CORES = 2
ROWS = 256
COLS = 256
BIG = 2.0 ** 100


def chip_offsets(chips):
    order = [0]
    for dist in range(1, chips // 2 + 1):
        order.append(dist)
        if 2 * dist != chips:
            order.append(-dist)
    return order


def normalise(raw):
    return raw * lax.rsqrt(jnp.sum(raw * raw, axis=-1, keepdims=True))


def kernel(group, temp_ref, q_hbm, d_hbm, w_hbm, qm_ref, dm_ref, lq_ref, ld_ref, lm_ref,
           q_in, d_in, w_in, q_buf, p_buf, bias, best, fin,
           q_sem, w_sem, d_sem, q_send, q_recv, relay_send, fin_send, fin_recv):
    pairs, q_len, hidden = q_in.shape
    d_len = dm_ref.shape[1]
    dim = w_in.shape[1]
    block = pairs * q_len
    chips = group // CORES
    offsets = chip_offsets(chips)
    tokens = group * block
    queries = group * pairs
    doc_rows = pairs * d_len
    tiles = doc_rows // ROWS

    me = lax.axis_index('data')
    chip = lax.div(me, CORES)
    core = lax.rem(me, CORES)
    partner = chip * CORES + (CORES - 1 - core)

    def at_offset(off):
        return lax.rem(chip + off + chips, chips)

    q_copy = pltpu.make_async_copy(q_hbm, q_in, q_sem)
    w_copy = pltpu.make_async_copy(w_hbm, w_in, w_sem)
    q_copy.start()
    w_copy.start()

    def d_copy(i):
        rows = pl.ds(pl.multiple_of(i * ROWS, ROWS), ROWS)
        return pltpu.make_async_copy(d_hbm.at[rows], d_in.at[rows], d_sem.at[i])

    for i in range(tiles):
        d_copy(i).start()

    barrier = pltpu.get_barrier_semaphore()
    for step in range(1, group):
        pl.semaphore_signal(barrier, inc=1, device_id={'data': lax.rem(me + step, group)}, device_id_type=MESH)

    row_pair = lax.broadcasted_iota(jnp.int32, (block, pairs), 0) // q_len
    picks = (row_pair == lax.broadcasted_iota(jnp.int32, (block, pairs), 1)).astype(jnp.bfloat16)
    spread = jnp.dot(picks, qm_ref[...].astype(jnp.float32).astype(jnp.bfloat16), preferred_element_type=jnp.float32)
    row_step = lax.broadcasted_iota(jnp.int32, (block, q_len), 0) % q_len
    own_step = row_step == lax.broadcasted_iota(jnp.int32, (block, q_len), 1)
    q_keep = jnp.sum(jnp.where(own_step, spread, 0.0), axis=1, keepdims=True)
    doc_bias = jnp.where(dm_ref[...] == 1, 0.0, -BIG)
    doc_bias = jnp.transpose(jnp.concatenate([doc_bias, jnp.zeros((128 - pairs, d_len), jnp.float32)], axis=0))
    for j in range(pairs):
        bias[j * d_len:(j + 1) * d_len, :] = jnp.broadcast_to(doc_bias[:, j:j + 1], (d_len, dim)).astype(jnp.bfloat16)

    q_copy.wait()
    w_copy.wait()
    q_raw = jnp.dot(q_in[...].reshape(block, hidden), w_in[...], preferred_element_type=jnp.float32)
    q_buf[0:block, :] = jnp.where(q_keep > 0.5, normalise(q_raw), 0.0).astype(jnp.bfloat16)

    def project(i):
        d_copy(i).wait()
        rows = pl.ds(pl.multiple_of(i * ROWS, ROWS), ROWS)
        raw = jnp.dot(d_in[rows, :], w_in[...], preferred_element_type=jnp.float32)
        p_buf[rows, :] = normalise(raw).astype(jnp.bfloat16)

    project(0)
    pl.semaphore_wait(barrier, group - 1)

    def slot(s):
        return q_buf.at[pl.ds(s * block, block), :]

    def to_partner():
        return pltpu.make_async_remote_copy(slot(0), slot(1), q_send.at[0], q_recv.at[1],
                                            device_id={'data': partner}, device_id_type=MESH)

    def to_chip(k):
        back = offsets.index(-offsets[k]) if -offsets[k] in offsets else k
        return pltpu.make_async_remote_copy(slot(0), slot(2 * back), q_send.at[k], q_recv.at[2 * back],
                                            device_id={'data': at_offset(offsets[k]) * CORES + core}, device_id_type=MESH)

    def relay(k):
        return pltpu.make_async_remote_copy(slot(2 * k), slot(2 * k + 1), relay_send.at[k], q_recv.at[2 * k + 1],
                                            device_id={'data': partner}, device_id_type=MESH)

    def arrival(s):
        return pltpu.make_async_remote_copy(slot(s), slot(s), q_send.at[0], q_recv.at[s],
                                            device_id={'data': partner}, device_id_type=MESH)

    to_partner().start()
    for k in range(1, chips):
        to_chip(k).start()

    def project_body(i, carry):
        project(i)
        return carry

    lax.fori_loop(1, tiles, project_body, 0)

    ones = (lax.broadcasted_iota(jnp.int32, (COLS, dim), 1) == 0).astype(jnp.bfloat16)
    ready = 1
    for n in range(tokens // COLS):
        last = (COLS * (n + 1) - 1) // block
        while ready <= last:
            arrival(ready).wait_recv()
            if ready % 2 == 0:
                relay(ready // 2).start()
            ready += 1
        rhs = jnp.concatenate([q_buf[n * COLS:(n + 1) * COLS, :], ones], axis=1)

        def score(j, carry):
            rows = pl.ds(pl.multiple_of(j * d_len, d_len), d_len)
            lhs = jnp.concatenate([p_buf[rows, :], bias[rows, :]], axis=1)
            sim = lax.dot_general(lhs, rhs, (((1,), (1,)), ((), ())), preferred_element_type=jnp.float32)
            best[pl.ds(j, 1), n * COLS:(n + 1) * COLS] = jnp.max(sim, axis=0, keepdims=True)
            return carry

        lax.fori_loop(0, pairs, score, 0)

    scores = jnp.zeros((pairs, queries), jnp.float32)
    for n in range(tokens // COLS):
        row = lax.broadcasted_iota(jnp.int32, (COLS, queries), 0) + n * COLS
        first, last = n * COLS // block, (COLS * (n + 1) - 1) // block
        start = None
        for s in range(first, last + 1):
            owner = at_offset(offsets[s // 2]) * CORES + (core if s % 2 == 0 else CORES - 1 - core)
            shift = owner * pairs - s * pairs
            start = shift if start is None else jnp.where(row >= s * block, shift, start)
        query = row // q_len + start
        picks = (query == lax.broadcasted_iota(jnp.int32, (COLS, queries), 1)).astype(jnp.bfloat16)
        part = best[:, n * COLS:(n + 1) * COLS]
        high = part.astype(jnp.bfloat16)
        rest = part - high.astype(jnp.float32)
        mid = rest.astype(jnp.bfloat16)
        low = (rest - mid.astype(jnp.float32)).astype(jnp.bfloat16)
        for piece in (low, mid, high):
            scores += jnp.dot(piece, picks, preferred_element_type=jnp.float32)

    z = scores / temp_ref[0]
    lane = lax.broadcasted_iota(jnp.int32, (pairs, queries), 1)
    sub = lax.broadcasted_iota(jnp.int32, (pairs, queries), 0)
    pos_grid = jnp.where(lane == me * pairs + sub, z, 0.0)
    pos_col = jnp.sum(pos_grid, axis=1, keepdims=True)
    pos_row = jnp.sum(pos_grid, axis=0, keepdims=True)
    col_max = jnp.max(z, axis=1, keepdims=True)
    lse_doc = jnp.log(jnp.sum(jnp.exp(z - col_max), axis=1, keepdims=True)) + col_max
    loss_doc = lse_doc - pos_col
    row_max = jnp.max(z, axis=0, keepdims=True)
    row_sum = jnp.sum(jnp.exp(z - row_max), axis=0, keepdims=True)
    doc_part = jnp.broadcast_to(jnp.sum(loss_doc - pos_col, axis=0, keepdims=True), (1, queries))
    fin[me] = jnp.concatenate([row_max, row_sum, doc_part, doc_part], axis=0)

    def share(step):
        to = lax.rem(me + step, group)
        return pltpu.make_async_remote_copy(fin.at[me], fin.at[me], fin_send.at[step - 1], fin_recv.at[step - 1],
                                            device_id={'data': to}, device_id_type=MESH)

    def shared(step):
        source = lax.rem(me - step + group, group)
        return pltpu.make_async_remote_copy(fin.at[source], fin.at[source], fin_send.at[step - 1], fin_recv.at[step - 1],
                                            device_id={'data': source}, device_id_type=MESH)

    for step in range(1, group):
        share(step).start()

    ld_ref[...] = jnp.sum(jnp.where(lane == sub, loss_doc, 0.0), axis=0, keepdims=True)[:, :pairs]

    to_partner().wait_send()
    for k in range(1, chips):
        to_chip(k).wait_send()
        relay(k).wait_send()
    for step in range(1, group):
        shared(step).wait_recv()

    every = fin[...]
    maxes, sums = every[:, 0, :], every[:, 1, :]
    top = jnp.max(maxes, axis=0, keepdims=True)
    lse_query = jnp.log(jnp.sum(sums * jnp.exp(maxes - top), axis=0, keepdims=True)) + top
    loss_query = lse_query - pos_row
    own = jnp.where(lane == me * pairs + sub, loss_query, 0.0)
    own = jnp.sum(own, axis=1, keepdims=True)
    lq_ref[...] = jnp.sum(jnp.where(lane == sub, own, 0.0), axis=0, keepdims=True)[:, :pairs]
    total = jnp.sum(lse_query, axis=1, keepdims=True) + jnp.sum(every[:, 2, :], axis=0, keepdims=True)[:, :1]
    lm_ref[...] = total / (2 * queries)

    for step in range(1, group):
        share(step).wait_send()


def solution(mesh):
    group = mesh.shape['data']
    batch_spec = P(('replica', 'data'))

    def local_loss(q_hidden, d_hidden, w_proj, q_mask, d_mask, temperature):
        pairs, q_len, hidden = q_hidden.shape
        d_len = d_hidden.shape[1]
        dim = w_proj.shape[1]
        block = pairs * q_len
        chips = group // CORES
        vmem = pl.BlockSpec(memory_space=pltpu.VMEM)
        hbm = pl.BlockSpec(memory_space=pl.ANY)
        out = pl.pallas_call(
            functools.partial(kernel, group),
            out_shape=[jax.ShapeDtypeStruct((1, pairs), jnp.float32), jax.ShapeDtypeStruct((1, pairs), jnp.float32),
                       jax.ShapeDtypeStruct((1, 1), jnp.float32)],
            in_specs=[pl.BlockSpec(memory_space=pltpu.SMEM), hbm, hbm, hbm, vmem, vmem],
            out_specs=[vmem, vmem, vmem],
            scratch_shapes=[
                pltpu.VMEM((pairs, q_len, hidden), jnp.bfloat16),
                pltpu.VMEM((pairs * d_len, hidden), jnp.bfloat16),
                pltpu.VMEM((hidden, dim), jnp.bfloat16),
                pltpu.VMEM((group * block, dim), jnp.bfloat16),
                pltpu.VMEM((pairs * d_len, dim), jnp.bfloat16),
                pltpu.VMEM((pairs * d_len, dim), jnp.bfloat16),
                pltpu.VMEM((pairs, group * block), jnp.float32),
                pltpu.VMEM((group, 4, group * pairs), jnp.float32),
                pltpu.SemaphoreType.DMA,
                pltpu.SemaphoreType.DMA,
                pltpu.SemaphoreType.DMA((pairs * d_len // ROWS,)),
                pltpu.SemaphoreType.DMA((chips,)),
                pltpu.SemaphoreType.DMA((group,)),
                pltpu.SemaphoreType.DMA((chips,)),
                pltpu.SemaphoreType.DMA((group - 1,)),
                pltpu.SemaphoreType.DMA((group - 1,)),
            ],
            compiler_params=pltpu.CompilerParams(collective_id=0, has_side_effects=True, vmem_limit_bytes=56 * 2 ** 20),
            name='late_interaction',
        )(temperature.reshape(1), q_hidden, d_hidden.reshape(pairs * d_len, hidden), w_proj, q_mask, d_mask)
        return out[0].reshape(pairs), out[1].reshape(pairs), out[2].reshape(1)

    return jax.shard_map(local_loss, mesh=mesh, in_specs=(batch_spec, batch_spec, P(), batch_spec, batch_spec, P()),
                         out_specs=(batch_spec, batch_spec, P('replica')), check_vma=False)
```

```python
import functools

import jax
import jax.numpy as jnp
from jax import lax
from jax.experimental import pallas as pl
from jax.experimental.pallas import tpu as pltpu
from jax.sharding import PartitionSpec as P

MESH = pl.DeviceIdType.MESH
CORES = 2
ROWS = 256
COLS = 256
BIG = 2.0 ** 100
EARLY = 2
GREET = 2
STEP = 2
LEAD = 2


def chip_offsets(chips):
    order = [0]
    for dist in range(1, chips // 2 + 1):
        order.append(dist)
        if 2 * dist != chips:
            order.append(-dist)
    return order


def normalise(raw):
    return raw * lax.rsqrt(jnp.sum(raw * raw, axis=-1, keepdims=True))


def kernel(group, temp_ref, q_hbm, d_hbm, w_hbm, qm_hbm, dm_hbm, lq_ref, ld_ref, lm_ref,
           q_in, d_in, w_in, qm_ref, dm_ref, q_buf, p_buf, bias, best, fin,
           q_sem, w_sem, qm_sem, dm_sem, d_sem, q_send, q_recv, relay_send, fin_send, fin_recv):
    pairs, q_len = qm_ref.shape
    hidden = q_in.shape[1]
    d_len = dm_ref.shape[1]
    dim = w_in.shape[1]
    block = pairs * q_len
    chips = group // CORES
    offsets = chip_offsets(chips)
    tokens = group * block
    queries = group * pairs
    doc_rows = pairs * d_len
    tiles = doc_rows // ROWS

    me = lax.axis_index('data')
    chip = lax.div(me, CORES)
    core = lax.rem(me, CORES)
    partner = chip * CORES + (CORES - 1 - core)

    def at_offset(off):
        return lax.rem(chip + off + chips, chips)

    w_copy = pltpu.make_async_copy(w_hbm, w_in, w_sem)
    q_copy = pltpu.make_async_copy(q_hbm, q_in, q_sem)
    qm_copy = pltpu.make_async_copy(qm_hbm, qm_ref, qm_sem)
    dm_copy = pltpu.make_async_copy(dm_hbm, dm_ref, dm_sem)

    def d_copy(i):
        rows = pl.ds(i * ROWS, ROWS)
        return pltpu.make_async_copy(d_hbm.at[rows], d_in.at[rows], d_sem.at[i])

    for copy in (qm_copy, w_copy, q_copy, dm_copy):
        copy.start()
    for i in range(EARLY):
        d_copy(i).start()

    barrier = pltpu.get_barrier_semaphore()
    for step in range(1, group):
        pl.semaphore_signal(barrier, inc=1, device_id={'data': lax.rem(me + step, group)}, device_id_type=MESH)

    with jax.named_scope('qmask'):
        qm_copy.wait()
        row_pair = lax.broadcasted_iota(jnp.int32, (block, pairs), 0) % pairs
        picks = (row_pair == lax.broadcasted_iota(jnp.int32, (block, pairs), 1)).astype(jnp.bfloat16)
        spread = jnp.dot(picks, qm_ref[...].astype(jnp.float32).astype(jnp.bfloat16), preferred_element_type=jnp.float32)
        row_step = lax.broadcasted_iota(jnp.int32, (block, q_len), 0) // pairs
        own_step = row_step == lax.broadcasted_iota(jnp.int32, (block, q_len), 1)
        q_keep = jnp.sum(jnp.where(own_step, spread, 0.0), axis=1, keepdims=True)
    with jax.named_scope('qproj'):
        w_copy.wait()
        q_copy.wait()
        for i in range(EARLY, tiles):
            d_copy(i).start()
        q_raw = jnp.dot(q_in[...], w_in[...], preferred_element_type=jnp.float32)
        q_buf[0:block, :] = jnp.where(q_keep > 0.5, normalise(q_raw), 0.0).astype(jnp.bfloat16)

    def project(i):
        rows = pl.ds(i * ROWS, ROWS)
        raw = jnp.dot(d_in[rows, :], w_in[...], preferred_element_type=jnp.float32)
        p_buf[rows, :] = normalise(raw).astype(jnp.bfloat16)

    def slot(s):
        return q_buf.at[pl.ds(s * block, block), :]

    def to_partner():
        return pltpu.make_async_remote_copy(slot(0), slot(1), q_send.at[0], q_recv.at[1],
                                            device_id={'data': partner}, device_id_type=MESH)

    def to_chip(k):
        back = offsets.index(-offsets[k]) if -offsets[k] in offsets else k
        return pltpu.make_async_remote_copy(slot(0), slot(2 * back), q_send.at[k], q_recv.at[2 * back],
                                            device_id={'data': at_offset(offsets[k]) * CORES + core}, device_id_type=MESH)

    def relay(k):
        return pltpu.make_async_remote_copy(slot(2 * k), slot(2 * k + 1), relay_send.at[k], q_recv.at[2 * k + 1],
                                            device_id={'data': partner}, device_id_type=MESH)

    def arrival(s):
        return pltpu.make_async_remote_copy(slot(s), slot(s), q_send.at[0], q_recv.at[s],
                                            device_id={'data': partner}, device_id_type=MESH)

    arrived = {0}

    def need(s):
        if s not in arrived:
            with jax.named_scope(f'need{s}'):
                arrival(s).wait_recv()
            arrived.add(s)

    def pass_on(k):
        need(2 * k)
        relay(k).start()

    with jax.named_scope('proj'):
        for i in range(tiles):
            if i == 1:
                with jax.named_scope('dmask'):
                    dm_copy.wait()
                    doc_bias = jnp.where(dm_ref[...] == 1, 0.0, -BIG)
                    doc_bias = jnp.concatenate([doc_bias, jnp.zeros((128 - pairs, d_len), jnp.float32)], axis=0)
                    doc_bias = jnp.transpose(doc_bias)
                    for j in range(pairs):
                        bias[j * d_len:(j + 1) * d_len, :] = jnp.broadcast_to(
                            doc_bias[:, j:j + 1], (d_len, dim)).astype(jnp.bfloat16)
            if i == GREET:
                with jax.named_scope('barrier'):
                    pl.semaphore_wait(barrier, group - 1)
                to_partner().start()
                for k in range(1, chips):
                    to_chip(k).start()
            if i % STEP == 0:
                for t in range(i, i + STEP):
                    d_copy(t).wait()
            project(i)
        pass_on(1)

    first_tile = [s * block // COLS for s in range(group)]
    ones = (lax.broadcasted_iota(jnp.int32, (COLS, dim), 1) == 0).astype(jnp.bfloat16)
    for n in range(tokens // COLS):
        for k in range(2, chips):
            if max(first_tile[2 * k + 1] - LEAD, 0) == n:
                pass_on(k)
        for s in range(group):
            if first_tile[s] == n:
                need(s)
        with jax.named_scope(f'score{n}'):
            rhs = jnp.concatenate([q_buf[n * COLS:(n + 1) * COLS, :], ones], axis=1)
            for j in range(0, pairs):
                rows = pl.ds(j * d_len, d_len)
                lhs = jnp.concatenate([p_buf[rows, :], bias[rows, :]], axis=1)
                sim = lax.dot_general(lhs, rhs, (((1,), (1,)), ((), ())), preferred_element_type=jnp.float32)
                best[pl.ds(j, 1), n * COLS:(n + 1) * COLS] = jnp.max(sim, axis=0, keepdims=True)

    with jax.named_scope('segsum'):
        scores = jnp.zeros((pairs, queries), jnp.float32)
        for n in range(tokens // COLS):
            row = lax.broadcasted_iota(jnp.int32, (COLS, queries), 0) + n * COLS
            first, last = n * COLS // block, (COLS * (n + 1) - 1) // block
            start = None
            for s in range(first, last + 1):
                owner = at_offset(offsets[s // 2]) * CORES + (core if s % 2 == 0 else CORES - 1 - core)
                start = owner * pairs if start is None else jnp.where(row >= s * block, owner * pairs, start)
            query = row % pairs + start
            picks = (query == lax.broadcasted_iota(jnp.int32, (COLS, queries), 1)).astype(jnp.bfloat16)
            part = best[:, n * COLS:(n + 1) * COLS]
            high = part.astype(jnp.bfloat16)
            rest = part - high.astype(jnp.float32)
            mid = rest.astype(jnp.bfloat16)
            low = (rest - mid.astype(jnp.float32)).astype(jnp.bfloat16)
            for piece in (low, mid, high):
                scores += jnp.dot(piece, picks, preferred_element_type=jnp.float32)

    with jax.named_scope('partial'):
        z = scores / temp_ref[0]
        lane = lax.broadcasted_iota(jnp.int32, (pairs, queries), 1)
        sub = lax.broadcasted_iota(jnp.int32, (pairs, queries), 0)
        pos_grid = jnp.where(lane == me * pairs + sub, z, 0.0)
        pos_col = jnp.sum(pos_grid, axis=1, keepdims=True)
        pos_row = jnp.sum(pos_grid, axis=0, keepdims=True)
        col_max = jnp.max(z, axis=1, keepdims=True)
        lse_doc = jnp.log(jnp.sum(jnp.exp(z - col_max), axis=1, keepdims=True)) + col_max
        loss_doc = lse_doc - pos_col
        row_max = jnp.max(z, axis=0, keepdims=True)
        row_sum = jnp.sum(jnp.exp(z - row_max), axis=0, keepdims=True)
        doc_part = jnp.broadcast_to(jnp.sum(loss_doc - pos_col, axis=0, keepdims=True), (1, queries))
        fin[me] = jnp.concatenate([row_max, row_sum, doc_part, doc_part], axis=0)

    def share(step):
        to = lax.rem(me + step, group)
        return pltpu.make_async_remote_copy(fin.at[me], fin.at[me], fin_send.at[step - 1], fin_recv.at[step - 1],
                                            device_id={'data': to}, device_id_type=MESH)

    def shared(step):
        source = lax.rem(me - step + group, group)
        return pltpu.make_async_remote_copy(fin.at[source], fin.at[source], fin_send.at[step - 1], fin_recv.at[step - 1],
                                            device_id={'data': source}, device_id_type=MESH)

    for step in range(1, group):
        share(step).start()

    ld_ref[...] = jnp.sum(jnp.where(lane == sub, loss_doc, 0.0), axis=0, keepdims=True)[:, :pairs]

    with jax.named_scope('shwait'):
        to_partner().wait_send()
        for k in range(1, chips):
            to_chip(k).wait_send()
            relay(k).wait_send()
        for step in range(1, group):
            shared(step).wait_recv()

    with jax.named_scope('finish'):
        every = fin[...]
        maxes, sums = every[:, 0, :], every[:, 1, :]
        top = jnp.max(maxes, axis=0, keepdims=True)
        lse_query = jnp.log(jnp.sum(sums * jnp.exp(maxes - top), axis=0, keepdims=True)) + top
        loss_query = lse_query - pos_row
        own = jnp.where(lane == me * pairs + sub, loss_query, 0.0)
        own = jnp.sum(own, axis=1, keepdims=True)
        lq_ref[...] = jnp.sum(jnp.where(lane == sub, own, 0.0), axis=0, keepdims=True)[:, :pairs]
        total = jnp.sum(lse_query, axis=1, keepdims=True) + jnp.sum(every[:, 2, :], axis=0, keepdims=True)[:, :1]
        lm_ref[...] = total / (2 * queries)

    for step in range(1, group):
        share(step).wait_send()


def solution(mesh):
    group = mesh.shape['data']
    batch_spec = P(('replica', 'data'))

    def local_loss(q_hidden, d_hidden, w_proj, q_mask, d_mask, temperature):
        pairs, q_len, hidden = q_hidden.shape
        d_len = d_hidden.shape[1]
        dim = w_proj.shape[1]
        block = pairs * q_len
        chips = group // CORES
        vmem = pl.BlockSpec(memory_space=pltpu.VMEM)
        hbm = pl.BlockSpec(memory_space=pl.ANY)
        out = pl.pallas_call(
            functools.partial(kernel, group),
            out_shape=[jax.ShapeDtypeStruct((1, pairs), jnp.float32), jax.ShapeDtypeStruct((1, pairs), jnp.float32),
                       jax.ShapeDtypeStruct((1, 1), jnp.float32)],
            in_specs=[pl.BlockSpec(memory_space=pltpu.SMEM), hbm, hbm, hbm, hbm, hbm],
            out_specs=[vmem, vmem, vmem],
            scratch_shapes=[
                pltpu.VMEM((block, hidden), jnp.bfloat16),
                pltpu.VMEM((pairs * d_len, hidden), jnp.bfloat16),
                pltpu.VMEM((hidden, dim), jnp.bfloat16),
                pltpu.VMEM((pairs, q_len), jnp.int32),
                pltpu.VMEM((pairs, d_len), jnp.int32),
                pltpu.VMEM((group * block, dim), jnp.bfloat16),
                pltpu.VMEM((pairs * d_len, dim), jnp.bfloat16),
                pltpu.VMEM((pairs * d_len, dim), jnp.bfloat16),
                pltpu.VMEM((pairs, group * block), jnp.float32),
                pltpu.VMEM((group, 4, group * pairs), jnp.float32),
                pltpu.SemaphoreType.DMA,
                pltpu.SemaphoreType.DMA,
                pltpu.SemaphoreType.DMA,
                pltpu.SemaphoreType.DMA,
                pltpu.SemaphoreType.DMA((pairs * d_len // ROWS,)),
                pltpu.SemaphoreType.DMA((chips,)),
                pltpu.SemaphoreType.DMA((group,)),
                pltpu.SemaphoreType.DMA((chips,)),
                pltpu.SemaphoreType.DMA((group - 1,)),
                pltpu.SemaphoreType.DMA((group - 1,)),
            ],
            compiler_params=pltpu.CompilerParams(collective_id=0, has_side_effects=True, vmem_limit_bytes=56 * 2 ** 20),
            name='late_interaction',
        )(temperature.reshape(1), q_hidden.transpose(1, 0, 2).reshape(block, hidden), d_hidden.reshape(pairs * d_len, hidden), w_proj, q_mask, d_mask)
        return out[0].reshape(pairs), out[1].reshape(pairs), out[2].reshape(1)

    return jax.shard_map(local_loss, mesh=mesh, in_specs=(batch_spec, batch_spec, P(), batch_spec, batch_spec, P()),
                         out_specs=(batch_spec, batch_spec, P('replica')), check_vma=False)
```

```python
import functools

import jax
import jax.numpy as jnp
from jax import lax
from jax.experimental import pallas as pl
from jax.experimental.pallas import tpu as pltpu
from jax.sharding import PartitionSpec as P

MESH = pl.DeviceIdType.MESH
CORES = 2
ROWS = 256
COLS = 256
BIG = 2.0 ** 100
EARLY = 3
GREET = 2
GROUPS = (2,3,3,4,4,4,2,2)
LOOK = False
RELAY = 6
FENCES = (0, 2, 4, 6, 8, 9)
DOCS = 1
LEAD = 2


def chip_offsets(chips):
    order = [0]
    for dist in range(1, chips // 2 + 1):
        order.append(dist)
        if 2 * dist != chips:
            order.append(-dist)
    return order


def normalise(raw):
    return raw * lax.rsqrt(jnp.sum(raw * raw, axis=-1, keepdims=True))


def kernel(group, temp_ref, q_hbm, d_hbm, w_hbm, qm_hbm, dm_hbm, out_ref,
           q_in, d_in, w_in, qm_ref, dm_ref, q_buf, p_buf, bias, dm_cols, best, grid, fin,
           q_sem, w_sem, qm_sem, dm_sem, d_sem, q_send, q_recv, relay_send, fin_send, fin_recv):
    pairs, q_len = qm_ref.shape
    hidden = q_in.shape[1]
    d_len = dm_ref.shape[1]
    dim = w_in.shape[1]
    block = pairs * q_len
    chips = group // CORES
    offsets = chip_offsets(chips)
    tokens = group * block
    queries = group * pairs
    doc_rows = pairs * d_len
    tiles = doc_rows // ROWS
    depth = hidden // COLS

    me = lax.axis_index('data')
    chip = lax.div(me, CORES)
    core = lax.rem(me, CORES)
    partner = chip * CORES + (CORES - 1 - core)

    def at_offset(off):
        return lax.rem(chip + off + chips, chips)

    w_copy = pltpu.make_async_copy(w_hbm, w_in, w_sem)
    q_copy = pltpu.make_async_copy(q_hbm, q_in, q_sem)
    qm_copy = pltpu.make_async_copy(qm_hbm, qm_ref, qm_sem)
    dm_copy = pltpu.make_async_copy(dm_hbm, dm_ref, dm_sem)

    def d_copy(i):
        rows = pl.ds(i * ROWS, ROWS)
        return pltpu.make_async_copy(d_hbm.at[rows], d_in.at[rows], d_sem.at[i])

    for copy in (w_copy, q_copy, qm_copy, dm_copy):
        copy.start()
    for i in range(EARLY):
        d_copy(i).start()

    barrier = pltpu.get_barrier_semaphore()
    for step in range(1, group):
        pl.semaphore_signal(barrier, inc=1, device_id={'data': lax.rem(me + step, group)}, device_id_type=MESH)

    with jax.named_scope('qproj'):
        w_copy.wait()
        q_copy.wait()
        for i in range(EARLY, tiles):
            d_copy(i).start()
        q_raw = jnp.dot(q_in[...], w_in[...], preferred_element_type=jnp.float32)
        qm_copy.wait()
        q_vecs = normalise(q_raw)
        for t in range(q_len):
            keep = jnp.broadcast_to(qm_ref[:, t:t + 1], (pairs, dim)) == 1
            grid[t * pairs:(t + 1) * pairs, :] = jnp.where(keep, q_vecs[t * pairs:(t + 1) * pairs, :], 0.0)
        q_buf[0:block, :] = grid[0:block, :].astype(jnp.bfloat16)

    def slot(s):
        return q_buf.at[pl.ds(s * block, block), :]

    def to_partner():
        return pltpu.make_async_remote_copy(slot(0), slot(1), q_send.at[0], q_recv.at[1],
                                            device_id={'data': partner}, device_id_type=MESH)

    def to_chip(k):
        back = offsets.index(-offsets[k]) if -offsets[k] in offsets else k
        return pltpu.make_async_remote_copy(slot(0), slot(2 * back), q_send.at[k], q_recv.at[2 * back],
                                            device_id={'data': at_offset(offsets[k]) * CORES + core}, device_id_type=MESH)

    def relay(k):
        return pltpu.make_async_remote_copy(slot(2 * k), slot(2 * k + 1), relay_send.at[k], q_recv.at[2 * k + 1],
                                            device_id={'data': partner}, device_id_type=MESH)

    def arrival(s):
        return pltpu.make_async_remote_copy(slot(s), slot(s), q_send.at[0], q_recv.at[s],
                                            device_id={'data': partner}, device_id_type=MESH)

    arrived = {0}

    def need(s):
        if s not in arrived:
            with jax.named_scope(f'need{s}'):
                arrival(s).wait_recv()
            arrived.add(s)

    def pass_on(k):
        need(2 * k)
        relay(k).start()

    def project(first, rows):
        raw = jnp.dot(d_in[first:first + rows, :], w_in[...], preferred_element_type=jnp.float32)
        p_buf[first:first + rows, :] = normalise(raw).astype(jnp.bfloat16)

    def mask(first, rows):
        for i in range(first, first + rows, ROWS):
            doc, start = divmod(i, d_len)
            bias[i:i + ROWS, :] = jnp.broadcast_to(
                dm_cols[start:start + ROWS, doc:doc + 1], (ROWS, dim)).astype(jnp.bfloat16)

    with jax.named_scope('proj'):
        starts = [sum(GROUPS[:g]) for g in range(len(GROUPS) + 1)]
        for g in range(len(GROUPS)):
            if g == GREET:
                with jax.named_scope('barrier'):
                    pl.semaphore_wait(barrier, group - 1)
                to_partner().start()
                for k in range(1, chips):
                    to_chip(k).start()
            if g == RELAY:
                pass_on(1)
            if LOOK:
                if g == 0:
                    for i in range(starts[1]):
                        d_copy(i).wait()
                if g + 1 < len(GROUPS):
                    for i in range(starts[g + 1], starts[g + 2]):
                        d_copy(i).wait()
            else:
                with jax.named_scope(f'dw{g}'):
                    for i in range(starts[g], starts[g + 1]):
                        d_copy(i).wait()
            for i in range(starts[g], starts[g + 1]):
                project(i * ROWS, ROWS)
            if g == 0:
                dm_copy.wait()
                masked = jnp.where(dm_ref[...] == 1, 0.0, -BIG)
                masked = jnp.concatenate([masked, jnp.zeros((128 - pairs, d_len), jnp.float32)], axis=0)
                dm_cols[...] = jnp.transpose(masked)
            else:
                mask(starts[g - 1] * ROWS, GROUPS[g - 1] * ROWS)
        mask(starts[-2] * ROWS, GROUPS[-1] * ROWS)

    ones = (lax.broadcasted_iota(jnp.int32, (COLS, dim), 1) == 0).astype(jnp.bfloat16)
    score_tiles = tokens // COLS
    first_tile = [s * block // COLS for s in range(group)]
    sums = {}

    def fetch(n):
        after = min([f for f in FENCES if f > n] + [score_tiles])
        later = min([f for f in FENCES if f > after] + [score_tiles])
        for s in range(group):
            if first_tile[s] < after and s % 2 == 0:
                need(s)
        for k in range(2, chips):
            if first_tile[2 * k + 1] < later and k not in passed:
                passed.add(k)
                pass_on(k)
        for s in range(group):
            if first_tile[s] < after:
                need(s)

    passed = set()

    def add_up(n):
        by_token = jnp.transpose(best[n % 2])
        for row in range(COLS // pairs):
            s = (n * COLS // pairs + row) // q_len
            term = by_token[row * pairs:(row + 1) * pairs, :]
            sums[s] = sums[s] + term if s in sums else term
        for s in [s for s in sums if (s + 1) * block <= (n + 1) * COLS]:
            owner = at_offset(offsets[s // 2]) * CORES + (core if s % 2 == 0 else CORES - 1 - core)
            grid[pl.ds(pl.multiple_of(owner * pairs, pairs), pairs), 0:pairs] = sums.pop(s)

    with jax.named_scope('scores'):
        for n in range(score_tiles):
            if n in FENCES:
                fetch(n)
            rhs = jnp.concatenate([q_buf[n * COLS:(n + 1) * COLS, :], ones], axis=1)
            for j in range(0, pairs, DOCS):
                rows = slice(j * d_len, (j + DOCS) * d_len)
                lhs = jnp.concatenate([p_buf[rows, :], bias[rows, :]], axis=1)
                sim = lax.dot_general(lhs, rhs, (((1,), (1,)), ((), ())), preferred_element_type=jnp.float32)
                for i in range(DOCS):
                    best[n % 2, j + i:j + i + 1, :] = jnp.max(sim[i * d_len:(i + 1) * d_len], axis=0, keepdims=True)
            if n:
                add_up(n - 1)
        add_up(score_tiles - 1)
    scores = jnp.transpose(grid[0:queries, 0:pairs])

    with jax.named_scope('partial'):
        z = scores / temp_ref[0]
        lane = lax.broadcasted_iota(jnp.int32, (pairs, queries), 1)
        sub = lax.broadcasted_iota(jnp.int32, (pairs, queries), 0)
        pos_grid = jnp.where(lane == me * pairs + sub, z, 0.0)
        pos_col = jnp.sum(pos_grid, axis=1, keepdims=True)
        pos_row = jnp.sum(pos_grid, axis=0, keepdims=True)
        col_max = jnp.max(z, axis=1, keepdims=True)
        lse_doc = jnp.log(jnp.sum(jnp.exp(z - col_max), axis=1, keepdims=True)) + col_max
        loss_doc = lse_doc - pos_col
        row_max = jnp.max(z, axis=0, keepdims=True)
        row_sum = jnp.sum(jnp.exp(z - row_max), axis=0, keepdims=True)
        doc_part = jnp.broadcast_to(jnp.sum(loss_doc - pos_col, axis=0, keepdims=True), (1, queries))
        fin[me] = jnp.concatenate([row_max, row_sum, doc_part, doc_part], axis=0)

    def share(step):
        to = lax.rem(me + step, group)
        return pltpu.make_async_remote_copy(fin.at[me], fin.at[me], fin_send.at[step - 1], fin_recv.at[step - 1],
                                            device_id={'data': to}, device_id_type=MESH)

    def shared(step):
        source = lax.rem(me - step + group, group)
        return pltpu.make_async_remote_copy(fin.at[source], fin.at[source], fin_send.at[step - 1], fin_recv.at[step - 1],
                                            device_id={'data': source}, device_id_type=MESH)

    for step in range(1, group):
        share(step).start()

    out_ref[1:2, 0:pairs] = jnp.sum(jnp.where(lane == sub, loss_doc, 0.0), axis=0, keepdims=True)[:, :pairs]

    with jax.named_scope('shwait'):
        to_partner().wait_send()
        for k in range(1, chips):
            to_chip(k).wait_send()
            relay(k).wait_send()
        for step in range(1, group):
            shared(step).wait_recv()

    with jax.named_scope('finish'):
        every = fin[...]
        maxes, sums = every[:, 0, :], every[:, 1, :]
        top = jnp.max(maxes, axis=0, keepdims=True)
        lse_query = jnp.log(jnp.sum(sums * jnp.exp(maxes - top), axis=0, keepdims=True)) + top
        loss_query = lse_query - pos_row
        own = jnp.where(lane == me * pairs + sub, loss_query, 0.0)
        own = jnp.sum(own, axis=1, keepdims=True)
        out_ref[0:1, 0:pairs] = jnp.sum(jnp.where(lane == sub, own, 0.0), axis=0, keepdims=True)[:, :pairs]
        total = jnp.sum(lse_query, axis=1, keepdims=True) + jnp.sum(every[:, 2, :], axis=0, keepdims=True)[:, :1]
        out_ref[2:3, 0:1] = total / (2 * queries)

    for step in range(1, group):
        share(step).wait_send()


def solution(mesh):
    group = mesh.shape['data']
    batch_spec = P(('replica', 'data'))

    def local_loss(q_hidden, d_hidden, w_proj, q_mask, d_mask, temperature):
        pairs, q_len, hidden = q_hidden.shape
        d_len = d_hidden.shape[1]
        dim = w_proj.shape[1]
        block = pairs * q_len
        chips = group // CORES
        vmem = pl.BlockSpec(memory_space=pltpu.VMEM)
        hbm = pl.BlockSpec(memory_space=pl.ANY)
        out = pl.pallas_call(
            functools.partial(kernel, group),
            out_shape=[jax.ShapeDtypeStruct((8, 128), jnp.float32)],
            in_specs=[pl.BlockSpec(memory_space=pltpu.SMEM), hbm, hbm, hbm, hbm, hbm],
            out_specs=[vmem],
            scratch_shapes=[
                pltpu.VMEM((block, hidden), jnp.bfloat16),
                pltpu.VMEM((pairs * d_len, hidden), jnp.bfloat16),
                pltpu.VMEM((hidden, dim), jnp.bfloat16),
                pltpu.VMEM((pairs, q_len), jnp.int32),
                pltpu.VMEM((pairs, d_len), jnp.int32),
                pltpu.VMEM((group * block, dim), jnp.bfloat16),
                pltpu.VMEM((pairs * d_len, dim), jnp.bfloat16),
                pltpu.VMEM((pairs * d_len, dim), jnp.bfloat16),
                pltpu.VMEM((d_len, 128), jnp.float32),
                pltpu.VMEM((2, pairs, COLS), jnp.float32),
                pltpu.VMEM((max(block, group * pairs), dim), jnp.float32),
                pltpu.VMEM((group, 4, group * pairs), jnp.float32),
                pltpu.SemaphoreType.DMA,
                pltpu.SemaphoreType.DMA,
                pltpu.SemaphoreType.DMA,
                pltpu.SemaphoreType.DMA,
                pltpu.SemaphoreType.DMA((pairs * d_len // ROWS,)),
                pltpu.SemaphoreType.DMA((chips,)),
                pltpu.SemaphoreType.DMA((group,)),
                pltpu.SemaphoreType.DMA((chips,)),
                pltpu.SemaphoreType.DMA((group - 1,)),
                pltpu.SemaphoreType.DMA((group - 1,)),
            ],
            compiler_params=pltpu.CompilerParams(collective_id=0, has_side_effects=True, vmem_limit_bytes=56 * 2 ** 20),
            name='late_interaction',
        )(temperature.reshape(1), q_hidden.transpose(1, 0, 2).reshape(block, hidden), d_hidden.reshape(pairs * d_len, hidden), w_proj, q_mask, d_mask)
        packed = out[0]
        def unpack(x_ref, q_ref, d_ref, m_ref):
            q_ref[...] = x_ref[0:1, 0:pairs]
            d_ref[...] = x_ref[1:2, 0:pairs]
            m_ref[...] = x_ref[2:3, 0:1]
        res = pl.pallas_call(unpack, out_shape=[jax.ShapeDtypeStruct((1, pairs), jnp.float32), jax.ShapeDtypeStruct((1, pairs), jnp.float32),
                       jax.ShapeDtypeStruct((1, 1), jnp.float32)], in_specs=[vmem], out_specs=[vmem, vmem, vmem], name='unpack')(packed)
        return res[0].reshape(pairs), res[1].reshape(pairs), res[2].reshape(1)

    return jax.shard_map(local_loss, mesh=mesh, in_specs=(batch_spec, batch_spec, P(), batch_spec, batch_spec, P()),
                         out_specs=(batch_spec, batch_spec, P('replica')), check_vma=False)
```

```python
import functools

import jax
import jax.numpy as jnp
from jax import lax
from jax.experimental import pallas as pl
from jax.experimental.pallas import tpu as pltpu
from jax.sharding import PartitionSpec as P

MESH = pl.DeviceIdType.MESH
CORES = 2
ROWS = 256
COLS = 256
BIG = 2.0 ** 100
EARLY = 3
ISSUED = (12,12,18,24,24,24)
DOCS = (1, 1, 2, 2, 2)
SENDS = (0, 0, 1, 2)
GREET_HIGH = 1
GREET_LOW = 2
HOME = 4
FENCES = (1,2,4,6,8)


def chip_offsets(chips):
    order = [0]
    for dist in range(1, chips // 2 + 1):
        order.append(dist)
        if 2 * dist != chips:
            order.append(-dist)
    return order


def slot_order(chips):
    direct, relayed = [0], [1]
    for first in range(1, chips, 2):
        count = min(2, chips - first)
        base = 2 * first
        direct += [base + i for i in range(count)]
        relayed += [base + count + i for i in range(count)]
    return direct, relayed


def normalise(raw):
    return raw * lax.rsqrt(jnp.sum(raw * raw, axis=-1, keepdims=True))


def kernel(group, temp_hbm, q_hbm, d_hbm, w_hbm, qm_hbm, dm_hbm, out_ref,
           temp_ref, q_in, d_in, w_in, qm_ref, dm_ref, q_buf, p_buf, bias, dm_cols, best, grid, fin,
           temp_sem, q_sem, w_sem, qm_sem, dm_sem, d_sem, q_send, q_recv, relay_send, fin_send, fin_recv):
    pairs, q_len = qm_ref.shape
    hidden = q_in.shape[1]
    d_len = dm_ref.shape[1]
    dim = w_in.shape[1]
    block = pairs * q_len
    chips = group // CORES
    offsets = chip_offsets(chips)
    direct, relayed = slot_order(chips)
    tokens = group * block
    queries = group * pairs
    doc_rows = pairs * d_len
    tiles = doc_rows // ROWS
    depth = hidden // COLS

    me = lax.axis_index('data')
    chip = lax.div(me, CORES)
    core = lax.rem(me, CORES)
    partner = chip * CORES + (CORES - 1 - core)

    def at_offset(off):
        return lax.rem(chip + off + chips, chips)

    w_copy = pltpu.make_async_copy(w_hbm, w_in, w_sem)
    q_copy = pltpu.make_async_copy(q_hbm, q_in, q_sem)
    qm_copy = pltpu.make_async_copy(qm_hbm, qm_ref, qm_sem)
    dm_copy = pltpu.make_async_copy(dm_hbm, dm_ref, dm_sem)
    temp_copy = pltpu.make_async_copy(temp_hbm, temp_ref, temp_sem)

    def d_copy(i):
        rows = pl.ds(i * ROWS, ROWS)
        return pltpu.make_async_copy(d_hbm.at[rows], d_in.at[rows], d_sem.at[i])

    for copy in (w_copy, q_copy, qm_copy, dm_copy):
        copy.start()
    for i in range(EARLY):
        d_copy(i).start()
    temp_copy.start()

    barrier = pltpu.get_barrier_semaphore()
    for step in range(1, group):
        pl.semaphore_signal(barrier, inc=1, device_id={'data': lax.rem(me + step, group)}, device_id_type=MESH)

    def slot(s):
        return q_buf.at[pl.ds(s * block, block), :]

    def to_partner():
        return pltpu.make_async_remote_copy(slot(0), slot(1), q_send.at[0], q_recv.at[1],
                                            device_id={'data': partner}, device_id_type=MESH)

    def to_chip(k):
        back = offsets.index(-offsets[k]) if -offsets[k] in offsets else k
        place = direct[back]
        return pltpu.make_async_remote_copy(slot(0), slot(place), q_send.at[k], q_recv.at[place],
                                            device_id={'data': at_offset(offsets[k]) * CORES + core}, device_id_type=MESH)

    def relay(k):
        return pltpu.make_async_remote_copy(slot(direct[k]), slot(relayed[k]), relay_send.at[k], q_recv.at[relayed[k]],
                                            device_id={'data': partner}, device_id_type=MESH)

    def arrival(s):
        return pltpu.make_async_remote_copy(slot(s), slot(s), q_send.at[0], q_recv.at[s],
                                            device_id={'data': partner}, device_id_type=MESH)

    arrived = {0}

    def need(s):
        if s not in arrived:
            with jax.named_scope(f'need{s}'):
                arrival(s).wait_recv()
            arrived.add(s)

    def pass_on(k):
        need(direct[k])
        relay(k).start()

    score_tiles = tokens // COLS
    first_tile = [s * block // COLS for s in range(group)]
    ones = (lax.broadcasted_iota(jnp.int32, (COLS, dim), 1) == 0).astype(jnp.bfloat16)

    def project_queries():
        q_vecs = normalise(jnp.dot(q_in[...], w_in[...], preferred_element_type=jnp.float32))
        for t in range(q_len):
            keep = jnp.broadcast_to(qm_ref[:, t:t + 1], (pairs, dim)) == 1
            grid[t * pairs:(t + 1) * pairs, :] = jnp.where(keep, q_vecs[t * pairs:(t + 1) * pairs, :], 0.0)
        q_buf[0:block, :] = grid[0:block, :].astype(jnp.bfloat16)

    def project(doc):
        for first in range(doc * d_len, (doc + 1) * d_len, ROWS):
            raw = jnp.dot(d_in[first:first + ROWS, :], w_in[...], preferred_element_type=jnp.float32)
            p_buf[first:first + ROWS, :] = normalise(raw).astype(jnp.bfloat16)

    def turn_masks():
        masked = jnp.where(dm_ref[...] == 1, 0.0, -BIG)
        masked = jnp.concatenate([masked, jnp.zeros((128 - pairs, d_len), jnp.float32)], axis=0)
        dm_cols[...] = jnp.transpose(masked)

    def mask(doc):
        bias[doc * d_len:(doc + 1) * d_len, :] = jnp.broadcast_to(
            dm_cols[:, doc:doc + 1], (d_len, dim)).astype(jnp.bfloat16)

    def score(n, docs):
        rhs = jnp.concatenate([q_buf[n * COLS:(n + 1) * COLS, :], ones], axis=1)
        for doc in docs:
            rows = slice(doc * d_len, (doc + 1) * d_len)
            lhs = jnp.concatenate([p_buf[rows, :], bias[rows, :]], axis=1)
            sim = lax.dot_general(lhs, rhs, (((1,), (1,)), ((), ())), preferred_element_type=jnp.float32)
            best[n % 2, doc:doc + 1, :] = jnp.max(sim, axis=0, keepdims=True)

    def send_later(turn):
        for k in range(1, chips):
            if SENDS[abs(offsets[k]) - 1] == turn:
                to_chip(k).start()

    def send_queries():
        with jax.named_scope('barrier'):
            pl.semaphore_wait(barrier, group - 1)
        to_partner().start()
        send_later(0)

    done = scored = 0
    with jax.named_scope('proj'):
        for step, count in enumerate(DOCS):
            if step == GREET_HIGH:
                pl.when(chip >= chips // 2)(send_queries)
            if step == GREET_LOW:
                pl.when(chip < chips // 2)(send_queries)
            for turn in range(1, max(SENDS) + 1):
                if step == GREET_HIGH + turn:
                    pl.when(chip >= chips // 2)(functools.partial(send_later, turn))
                if step == GREET_LOW + turn:
                    pl.when(chip < chips // 2)(functools.partial(send_later, turn))
            if step == HOME:
                need(1)
            if step == 0:
                with jax.named_scope('dmaw'):
                    w_copy.wait()
                    q_copy.wait()
                    for i in range(EARLY, ISSUED[0]):
                        d_copy(i).start()
                    qm_copy.wait()
                    dm_copy.wait()
            for i in range(ISSUED[step], ISSUED[step + 1]):
                d_copy(i).start()
            with jax.named_scope(f'dw{step}'):
                for i in range(done * d_len // ROWS, (done + count) * d_len // ROWS):
                    d_copy(i).wait()
            if step == 0:
                project_queries()
                turn_masks()
            for doc in range(done, done + count):
                project(doc)
            if step >= HOME:
                score(0, range(scored, done))
                scored = done
            for doc in range(done, done + count):
                mask(doc)
            done += count

    sums = {}

    def fetch(n):
        after = min([f for f in FENCES if f > n] + [score_tiles])
        later = min([f for f in FENCES if f > after] + [score_tiles])
        for s in range(group):
            if first_tile[s] < after and s in direct:
                need(s)
        for k in range(1, chips):
            if first_tile[relayed[k]] < later and k not in passed:
                passed.add(k)
                pass_on(k)
        for s in range(group):
            if first_tile[s] < after:
                need(s)

    passed = set()

    def add_up(n):
        by_token = jnp.transpose(best[n % 2])
        for row in range(COLS // pairs):
            s = (n * COLS // pairs + row) // q_len
            term = by_token[row * pairs:(row + 1) * pairs, :]
            sums[s] = sums[s] + term if s in sums else term
        for s in [s for s in sums if (s + 1) * block <= (n + 1) * COLS]:
            place = direct if s in direct else relayed
            owner = at_offset(offsets[place.index(s)]) * CORES + (core if s in direct else CORES - 1 - core)
            grid[pl.ds(pl.multiple_of(owner * pairs, pairs), pairs), 0:pairs] = sums.pop(s)

    with jax.named_scope('scores'):
        for n in range(1, score_tiles):
            if n in FENCES:
                fetch(n)
            if n == 1:
                score(0, range(scored, pairs))
            score(n, range(pairs))
            add_up(n - 1)
        add_up(score_tiles - 1)
    scores = jnp.transpose(grid[0:queries, 0:pairs])

    with jax.named_scope('partial'):
        temp_copy.wait()
        z = scores / temp_ref[0]
        lane = lax.broadcasted_iota(jnp.int32, (pairs, queries), 1)
        sub = lax.broadcasted_iota(jnp.int32, (pairs, queries), 0)
        pos_grid = jnp.where(lane == me * pairs + sub, z, 0.0)
        pos_col = jnp.sum(pos_grid, axis=1, keepdims=True)
        pos_row = jnp.sum(pos_grid, axis=0, keepdims=True)
        col_max = jnp.max(z, axis=1, keepdims=True)
        lse_doc = jnp.log(jnp.sum(jnp.exp(z - col_max), axis=1, keepdims=True)) + col_max
        loss_doc = lse_doc - pos_col
        row_max = jnp.max(z, axis=0, keepdims=True)
        row_sum = jnp.sum(jnp.exp(z - row_max), axis=0, keepdims=True)
        doc_part = jnp.broadcast_to(jnp.sum(loss_doc - pos_col, axis=0, keepdims=True), (1, queries))
        fin[me] = jnp.concatenate([row_max, row_sum, doc_part, doc_part], axis=0)

    def share(step):
        to = lax.rem(me + step, group)
        return pltpu.make_async_remote_copy(fin.at[me], fin.at[me], fin_send.at[step - 1], fin_recv.at[step - 1],
                                            device_id={'data': to}, device_id_type=MESH)

    def shared(step):
        source = lax.rem(me - step + group, group)
        return pltpu.make_async_remote_copy(fin.at[source], fin.at[source], fin_send.at[step - 1], fin_recv.at[step - 1],
                                            device_id={'data': source}, device_id_type=MESH)

    for step in sorted(range(1, group), key=lambda step: abs(2 * step - group)):
        share(step).start()

    out_ref[1:2, 0:pairs] = jnp.sum(jnp.where(lane == sub, loss_doc, 0.0), axis=0, keepdims=True)[:, :pairs]

    with jax.named_scope('shwait'):
        to_partner().wait_send()
        for k in range(1, chips):
            to_chip(k).wait_send()
            relay(k).wait_send()
        for step in range(1, group):
            shared(step).wait_recv()

    with jax.named_scope('finish'):
        every = fin[...]
        maxes, sums = every[:, 0, :], every[:, 1, :]
        top = jnp.max(maxes, axis=0, keepdims=True)
        lse_query = jnp.log(jnp.sum(sums * jnp.exp(maxes - top), axis=0, keepdims=True)) + top
        loss_query = lse_query - pos_row
        own = jnp.where(lane == me * pairs + sub, loss_query, 0.0)
        own = jnp.sum(own, axis=1, keepdims=True)
        out_ref[0:1, 0:pairs] = jnp.sum(jnp.where(lane == sub, own, 0.0), axis=0, keepdims=True)[:, :pairs]
        total = jnp.sum(lse_query, axis=1, keepdims=True) + jnp.sum(every[:, 2, :], axis=0, keepdims=True)[:, :1]
        out_ref[2:3, 0:1] = total / (2 * queries)

    for step in range(1, group):
        share(step).wait_send()


def solution(mesh):
    group = mesh.shape['data']
    batch_spec = P(('replica', 'data'))

    def local_loss(q_hidden, d_hidden, w_proj, q_mask, d_mask, temperature):
        pairs, q_len, hidden = q_hidden.shape
        d_len = d_hidden.shape[1]
        dim = w_proj.shape[1]
        block = pairs * q_len
        chips = group // CORES
        vmem = pl.BlockSpec(memory_space=pltpu.VMEM)
        hbm = pl.BlockSpec(memory_space=pl.ANY)
        out = pl.pallas_call(
            functools.partial(kernel, group),
            out_shape=[jax.ShapeDtypeStruct((8, 128), jnp.float32)],
            in_specs=[hbm, hbm, hbm, hbm, hbm, hbm],
            out_specs=[vmem],
            scratch_shapes=[
                pltpu.SMEM((1,), jnp.float32),
                pltpu.VMEM((block, hidden), jnp.bfloat16),
                pltpu.VMEM((pairs * d_len, hidden), jnp.bfloat16),
                pltpu.VMEM((hidden, dim), jnp.bfloat16),
                pltpu.VMEM((pairs, q_len), jnp.int32),
                pltpu.VMEM((pairs, d_len), jnp.int32),
                pltpu.VMEM((group * block, dim), jnp.bfloat16),
                pltpu.VMEM((pairs * d_len, dim), jnp.bfloat16),
                pltpu.VMEM((pairs * d_len, dim), jnp.bfloat16),
                pltpu.VMEM((d_len, 128), jnp.float32),
                pltpu.VMEM((2, pairs, COLS), jnp.float32),
                pltpu.VMEM((max(block, group * pairs), dim), jnp.float32),
                pltpu.VMEM((group, 4, group * pairs), jnp.float32),
                pltpu.SemaphoreType.DMA,
                pltpu.SemaphoreType.DMA,
                pltpu.SemaphoreType.DMA,
                pltpu.SemaphoreType.DMA,
                pltpu.SemaphoreType.DMA,
                pltpu.SemaphoreType.DMA((pairs * d_len // ROWS,)),
                pltpu.SemaphoreType.DMA((chips,)),
                pltpu.SemaphoreType.DMA((group,)),
                pltpu.SemaphoreType.DMA((chips,)),
                pltpu.SemaphoreType.DMA((group - 1,)),
                pltpu.SemaphoreType.DMA((group - 1,)),
            ],
            compiler_params=pltpu.CompilerParams(collective_id=0, has_side_effects=True, vmem_limit_bytes=56 * 2 ** 20),
            name='late_interaction',
        )(temperature.reshape(1), q_hidden.transpose(1, 0, 2).reshape(block, hidden), d_hidden.reshape(pairs * d_len, hidden), w_proj, q_mask, d_mask)
        packed = out[0]
        def unpack(x_ref, q_ref, d_ref, m_ref):
            q_ref[...] = x_ref[0:1, 0:pairs]
            d_ref[...] = x_ref[1:2, 0:pairs]
            m_ref[...] = x_ref[2:3, 0:1]
        res = pl.pallas_call(unpack, out_shape=[jax.ShapeDtypeStruct((1, pairs), jnp.float32), jax.ShapeDtypeStruct((1, pairs), jnp.float32),
                       jax.ShapeDtypeStruct((1, 1), jnp.float32)], in_specs=[vmem], out_specs=[vmem, vmem, vmem], name='unpack')(packed)
        return res[0].reshape(pairs), res[1].reshape(pairs), res[2].reshape(1)

    return jax.shard_map(local_loss, mesh=mesh, in_specs=(batch_spec, batch_spec, P(), batch_spec, batch_spec, P()),
                         out_specs=(batch_spec, batch_spec, P('replica')), check_vma=False)
```

```python
import functools

import jax
import jax.numpy as jnp
from jax import lax
from jax.experimental import pallas as pl
from jax.experimental.pallas import tpu as pltpu
from jax.sharding import PartitionSpec as P

MESH = pl.DeviceIdType.MESH
CORES = 2
ROWS = 256
COLS = 256
BIG = 2.0 ** 100
VMEM = 56552448
APART = True
SOON = 6
EARLY = 3
ISSUED = (12,12,18,24,24,24)
DOCS = (1, 1, 2, 2, 2)
SENDS = (0, 0, 1, 2)
GREET_HIGH = 1
GREET_LOW = 2
HOME = 4
FENCES = (1,2,4,6,8)


def chip_offsets(chips):
    order = [0]
    for dist in range(1, chips // 2 + 1):
        order.append(dist)
        if 2 * dist != chips:
            order.append(-dist)
    return order


def slot_order(chips):
    direct, relayed = [0], [1]
    for first in range(1, chips, 2):
        count = min(2, chips - first)
        base = 2 * first
        direct += [base + i for i in range(count)]
        relayed += [base + count + i for i in range(count)]
    return direct, relayed


def normalise(raw):
    return raw * lax.rsqrt(jnp.sum(raw * raw, axis=-1, keepdims=True))


def kernel(group, temp_hbm, q_hbm, d_hbm, w_hbm, qm_hbm, dm_hbm, out_ref,
           temp_ref, q_in, d_in, w_in, qm_ref, dm_ref, q_buf, p_buf, bias, dm_cols, best, grid, fin,
           temp_sem, q_sem, w_sem, qm_sem, dm_sem, d_sem, q_send, q_recv, relay_send, fin_send, fin_recv):
    pairs, q_len = qm_ref.shape
    hidden = q_in.shape[1]
    d_len = dm_ref.shape[1]
    dim = w_in.shape[1]
    block = pairs * q_len
    chips = group // CORES
    offsets = chip_offsets(chips)
    direct, relayed = slot_order(chips)
    tokens = group * block
    queries = group * pairs
    doc_rows = pairs * d_len
    tiles = doc_rows // ROWS
    depth = hidden // COLS

    me = lax.axis_index('data')
    chip = lax.div(me, CORES)
    core = lax.rem(me, CORES)
    partner = chip * CORES + (CORES - 1 - core)

    def at_offset(off):
        return lax.rem(chip + off + chips, chips)

    w_copy = pltpu.make_async_copy(w_hbm, w_in, w_sem)
    q_copy = pltpu.make_async_copy(q_hbm, q_in, q_sem)
    qm_copy = pltpu.make_async_copy(qm_hbm, qm_ref, qm_sem)
    dm_copy = pltpu.make_async_copy(dm_hbm, dm_ref, dm_sem)
    temp_copy = pltpu.make_async_copy(temp_hbm, temp_ref, temp_sem)

    def d_copy(i):
        rows = pl.ds(i * ROWS, ROWS)
        return pltpu.make_async_copy(d_hbm.at[rows], d_in.at[rows], d_sem.at[i])

    for copy in (w_copy, q_copy, qm_copy, dm_copy):
        copy.start()
    for i in range(EARLY):
        d_copy(i).start()
    temp_copy.start()

    barrier = pltpu.get_barrier_semaphore()
    for step in range(1, group):
        pl.semaphore_signal(barrier, inc=1, device_id={'data': lax.rem(me + step, group)}, device_id_type=MESH)

    def slot(s):
        return q_buf.at[pl.ds(s * block, block), :]

    def to_partner():
        return pltpu.make_async_remote_copy(slot(0), slot(1), q_send.at[0], q_recv.at[1],
                                            device_id={'data': partner}, device_id_type=MESH)

    def to_chip(k):
        back = offsets.index(-offsets[k]) if -offsets[k] in offsets else k
        place = direct[back]
        return pltpu.make_async_remote_copy(slot(0), slot(place), q_send.at[k], q_recv.at[place],
                                            device_id={'data': at_offset(offsets[k]) * CORES + core}, device_id_type=MESH)

    def relay(k):
        return pltpu.make_async_remote_copy(slot(direct[k]), slot(relayed[k]), relay_send.at[k], q_recv.at[relayed[k]],
                                            device_id={'data': partner}, device_id_type=MESH)

    def arrival(s):
        return pltpu.make_async_remote_copy(slot(s), slot(s), q_send.at[0], q_recv.at[s],
                                            device_id={'data': partner}, device_id_type=MESH)

    arrived = {0}

    def need(s):
        if s not in arrived:
            with jax.named_scope(f'need{s}'):
                arrival(s).wait_recv()
            arrived.add(s)

    def pass_on(k):
        need(direct[k])
        relay(k).start()

    score_tiles = tokens // COLS
    first_tile = [s * block // COLS for s in range(group)]
    ones = (lax.broadcasted_iota(jnp.int32, (COLS, dim), 1) == 0).astype(jnp.bfloat16)

    def project_queries():
        q_vecs = normalise(jnp.dot(q_in[...], w_in[...], preferred_element_type=jnp.float32))
        for t in range(q_len):
            keep = jnp.broadcast_to(qm_ref[:, t:t + 1], (pairs, dim)) == 1
            grid[t * pairs:(t + 1) * pairs, :] = jnp.where(keep, q_vecs[t * pairs:(t + 1) * pairs, :], 0.0)
        q_buf[0:block, :] = grid[0:block, :].astype(jnp.bfloat16)

    def project(doc):
        for first in range(doc * d_len, (doc + 1) * d_len, ROWS):
            raw = jnp.dot(d_in[first:first + ROWS, :], w_in[...], preferred_element_type=jnp.float32)
            p_buf[first:first + ROWS, :] = normalise(raw).astype(jnp.bfloat16)

    def turn_masks():
        masked = jnp.where(dm_ref[...] == 1, 0.0, -BIG)
        masked = jnp.concatenate([masked, jnp.zeros((128 - pairs, d_len), jnp.float32)], axis=0)
        dm_cols[...] = jnp.transpose(masked)

    def mask(doc):
        bias[doc * d_len:(doc + 1) * d_len, :] = jnp.broadcast_to(
            dm_cols[:, doc:doc + 1], (d_len, dim)).astype(jnp.bfloat16)

    def score(n, docs):
        rhs = jnp.concatenate([q_buf[n * COLS:(n + 1) * COLS, :], ones], axis=1)
        for doc in docs:
            rows = slice(doc * d_len, (doc + 1) * d_len)
            lhs = jnp.concatenate([p_buf[rows, :], bias[rows, :]], axis=1)
            sim = lax.dot_general(lhs, rhs, (((1,), (1,)), ((), ())), preferred_element_type=jnp.float32)
            best[n % 2, doc:doc + 1, :] = jnp.max(sim, axis=0, keepdims=True)

    def send_later(turn):
        for k in range(1, chips):
            if SENDS[abs(offsets[k]) - 1] == turn:
                to_chip(k).start()

    def send_queries():
        with jax.named_scope('barrier'):
            pl.semaphore_wait(barrier, group - 1)
        to_partner().start()
        send_later(0)

    done = scored = 0
    with jax.named_scope('proj'):
        for step, count in enumerate(DOCS):
            if step == GREET_HIGH:
                pl.when(chip >= chips // 2)(send_queries)
            if step == GREET_LOW:
                pl.when(chip < chips // 2)(send_queries)
            for turn in range(1, max(SENDS) + 1):
                if step == GREET_HIGH + turn:
                    pl.when(chip >= chips // 2)(functools.partial(send_later, turn))
                if step == GREET_LOW + turn:
                    pl.when(chip < chips // 2)(functools.partial(send_later, turn))
            if step == HOME:
                need(1)
            if step == 0:
                with jax.named_scope('dmaw'):
                    w_copy.wait()
                    for i in range(EARLY, SOON):
                        d_copy(i).start()
                    q_copy.wait()
                    for i in range(SOON, ISSUED[0]):
                        d_copy(i).start()
                    qm_copy.wait()
                    dm_copy.wait()
                    if APART:
                        project_queries()
                        turn_masks()
            for i in range(ISSUED[step], ISSUED[step + 1]):
                d_copy(i).start()
            with jax.named_scope(f'dw{step}'):
                for i in range(done * d_len // ROWS, (done + count) * d_len // ROWS):
                    d_copy(i).wait()
            if step == 0 and not APART:
                project_queries()
                turn_masks()
            for doc in range(done, done + count):
                project(doc)
            if step >= HOME:
                score(0, range(scored, done))
                scored = done
            for doc in range(done, done + count):
                mask(doc)
            done += count

    sums = {}

    def fetch(n):
        after = min([f for f in FENCES if f > n] + [score_tiles])
        later = min([f for f in FENCES if f > after] + [score_tiles])
        for s in range(group):
            if first_tile[s] < after and s in direct:
                need(s)
        for k in range(1, chips):
            if first_tile[relayed[k]] < later and k not in passed:
                passed.add(k)
                pass_on(k)
        for s in range(group):
            if first_tile[s] < after:
                need(s)

    passed = set()

    def add_up(n):
        by_token = jnp.transpose(best[n % 2])
        for row in range(COLS // pairs):
            s = (n * COLS // pairs + row) // q_len
            term = by_token[row * pairs:(row + 1) * pairs, :]
            sums[s] = sums[s] + term if s in sums else term
        for s in [s for s in sums if (s + 1) * block <= (n + 1) * COLS]:
            place = direct if s in direct else relayed
            owner = at_offset(offsets[place.index(s)]) * CORES + (core if s in direct else CORES - 1 - core)
            grid[pl.ds(pl.multiple_of(owner * pairs, pairs), pairs), 0:pairs] = sums.pop(s)

    with jax.named_scope('scores'):
        for n in range(1, score_tiles):
            if n in FENCES:
                fetch(n)
            if n == 1:
                score(0, range(scored, pairs))
            score(n, range(pairs))
            add_up(n - 1)
        add_up(score_tiles - 1)
    scores = jnp.transpose(grid[0:queries, 0:pairs])

    with jax.named_scope('partial'):
        temp_copy.wait()
        z = scores / temp_ref[0]
        lane = lax.broadcasted_iota(jnp.int32, (pairs, queries), 1)
        sub = lax.broadcasted_iota(jnp.int32, (pairs, queries), 0)
        pos_grid = jnp.where(lane == me * pairs + sub, z, 0.0)
        pos_col = jnp.sum(pos_grid, axis=1, keepdims=True)
        pos_row = jnp.sum(pos_grid, axis=0, keepdims=True)
        col_max = jnp.max(z, axis=1, keepdims=True)
        lse_doc = jnp.log(jnp.sum(jnp.exp(z - col_max), axis=1, keepdims=True)) + col_max
        loss_doc = lse_doc - pos_col
        row_max = jnp.max(z, axis=0, keepdims=True)
        row_sum = jnp.sum(jnp.exp(z - row_max), axis=0, keepdims=True)
        doc_part = jnp.broadcast_to(jnp.sum(loss_doc - pos_col, axis=0, keepdims=True), (1, queries))
        fin[me] = jnp.concatenate([row_max, row_sum, doc_part, doc_part], axis=0)

    def share(step):
        to = lax.rem(me + step, group)
        return pltpu.make_async_remote_copy(fin.at[me], fin.at[me], fin_send.at[step - 1], fin_recv.at[step - 1],
                                            device_id={'data': to}, device_id_type=MESH)

    def shared(step):
        source = lax.rem(me - step + group, group)
        return pltpu.make_async_remote_copy(fin.at[source], fin.at[source], fin_send.at[step - 1], fin_recv.at[step - 1],
                                            device_id={'data': source}, device_id_type=MESH)

    for step in sorted(range(1, group), key=lambda step: abs(2 * step - group)):
        share(step).start()

    out_ref[1:2, 0:pairs] = jnp.sum(jnp.where(lane == sub, loss_doc, 0.0), axis=0, keepdims=True)[:, :pairs]

    with jax.named_scope('shwait'):
        to_partner().wait_send()
        for k in range(1, chips):
            to_chip(k).wait_send()
            relay(k).wait_send()
        for step in range(1, group):
            shared(step).wait_recv()

    with jax.named_scope('finish'):
        every = fin[...]
        maxes, sums = every[:, 0, :], every[:, 1, :]
        top = jnp.max(maxes, axis=0, keepdims=True)
        lse_query = jnp.log(jnp.sum(sums * jnp.exp(maxes - top), axis=0, keepdims=True)) + top
        loss_query = lse_query - pos_row
        own = jnp.where(lane == me * pairs + sub, loss_query, 0.0)
        own = jnp.sum(own, axis=1, keepdims=True)
        out_ref[0:1, 0:pairs] = jnp.sum(jnp.where(lane == sub, own, 0.0), axis=0, keepdims=True)[:, :pairs]
        total = jnp.sum(lse_query, axis=1, keepdims=True) + jnp.sum(every[:, 2, :], axis=0, keepdims=True)[:, :1]
        out_ref[2:3, 0:1] = total / (2 * queries)

    for step in range(1, group):
        share(step).wait_send()


def solution(mesh):
    group = mesh.shape['data']
    batch_spec = P(('replica', 'data'))

    def local_loss(q_hidden, d_hidden, w_proj, q_mask, d_mask, temperature):
        pairs, q_len, hidden = q_hidden.shape
        d_len = d_hidden.shape[1]
        dim = w_proj.shape[1]
        block = pairs * q_len
        chips = group // CORES
        vmem = pl.BlockSpec(memory_space=pltpu.VMEM)
        hbm = pl.BlockSpec(memory_space=pltpu.HBM)
        out = pl.pallas_call(
            functools.partial(kernel, group),
            out_shape=[jax.ShapeDtypeStruct((8, 128), jnp.float32)],
            in_specs=[hbm, hbm, hbm, hbm, hbm, hbm],
            out_specs=[vmem],
            scratch_shapes=[
                pltpu.SMEM((1,), jnp.float32),
                pltpu.VMEM((block, hidden), jnp.bfloat16),
                pltpu.VMEM((pairs * d_len, hidden), jnp.bfloat16),
                pltpu.VMEM((hidden, dim), jnp.bfloat16),
                pltpu.VMEM((pairs, q_len), jnp.int32),
                pltpu.VMEM((pairs, d_len), jnp.int32),
                pltpu.VMEM((group * block, dim), jnp.bfloat16),
                pltpu.VMEM((pairs * d_len, dim), jnp.bfloat16),
                pltpu.VMEM((pairs * d_len, dim), jnp.bfloat16),
                pltpu.VMEM((d_len, 128), jnp.float32),
                pltpu.VMEM((2, pairs, COLS), jnp.float32),
                pltpu.VMEM((max(block, group * pairs), dim), jnp.float32),
                pltpu.VMEM((group, 4, group * pairs), jnp.float32),
                pltpu.SemaphoreType.DMA,
                pltpu.SemaphoreType.DMA,
                pltpu.SemaphoreType.DMA,
                pltpu.SemaphoreType.DMA,
                pltpu.SemaphoreType.DMA,
                pltpu.SemaphoreType.DMA((pairs * d_len // ROWS,)),
                pltpu.SemaphoreType.DMA((chips,)),
                pltpu.SemaphoreType.DMA((group,)),
                pltpu.SemaphoreType.DMA((chips,)),
                pltpu.SemaphoreType.DMA((group - 1,)),
                pltpu.SemaphoreType.DMA((group - 1,)),
            ],
            compiler_params=pltpu.CompilerParams(collective_id=0, has_side_effects=True, vmem_limit_bytes=VMEM),
            name='late_interaction',
        )(temperature.reshape(1), q_hidden.transpose(1, 0, 2).reshape(block, hidden), d_hidden.reshape(pairs * d_len, hidden), w_proj, q_mask, d_mask)
        packed = out[0]
        def unpack(x_ref, q_ref, d_ref, m_ref):
            q_ref[...] = x_ref[0:1, 0:pairs]
            d_ref[...] = x_ref[1:2, 0:pairs]
            m_ref[...] = x_ref[2:3, 0:1]
        res = pl.pallas_call(unpack, out_shape=[jax.ShapeDtypeStruct((1, pairs), jnp.float32), jax.ShapeDtypeStruct((1, pairs), jnp.float32),
                       jax.ShapeDtypeStruct((1, 1), jnp.float32)], in_specs=[vmem], out_specs=[vmem, vmem, vmem],
                       compiler_params=pltpu.CompilerParams(vmem_limit_bytes=2 ** 20), name='unpack')(packed)
        return res[0].reshape(pairs), res[1].reshape(pairs), res[2].reshape(1)

    return jax.shard_map(local_loss, mesh=mesh, in_specs=(batch_spec, batch_spec, P(), batch_spec, batch_spec, P()),
                         out_specs=(batch_spec, batch_spec, P('replica')), check_vma=False)
```

```python
import functools

import jax
import jax.numpy as jnp
from jax import lax
from jax.experimental import pallas as pl
from jax.experimental.pallas import tpu as pltpu
from jax.sharding import PartitionSpec as P

MESH = pl.DeviceIdType.MESH
CORES = 2
ROWS = 256
COLS = 256
BIG = 2.0 ** 100
VMEM = 56552448
APART = True
SOON = 6
EARLY = 3
ISSUED = (12,12,18,24,24,24)
DOCS = (1, 1, 2, 2, 2)
SENDS = (0, 0, 1, 2)
GREET_HIGH = 1
GREET_LOW = 2
HOME = 4
FENCES = (1,2,4,6,8)


def chip_offsets(chips):
    order = [0]
    for dist in range(1, chips // 2 + 1):
        order.append(dist)
        if 2 * dist != chips:
            order.append(-dist)
    return order


def slot_order(chips):
    direct, relayed = [0], [1]
    for first in range(1, chips, 2):
        count = min(2, chips - first)
        base = 2 * first
        direct += [base + i for i in range(count)]
        relayed += [base + count + i for i in range(count)]
    return direct, relayed


def normalise(raw):
    return raw * lax.rsqrt(jnp.sum(raw * raw, axis=-1, keepdims=True))


def kernel(group, temp_hbm, q_hbm, d_hbm, w_hbm, qm_hbm, dm_hbm, out_ref,
           temp_ref, q_in, d_in, w_in, qm_ref, dm_ref, q_buf, p_buf, bias, dm_cols, best, grid, fin,
           temp_sem, q_sem, w_sem, qm_sem, dm_sem, d_sem, q_send, q_recv, relay_send, fin_send, fin_recv):
    pairs, q_len = qm_ref.shape
    hidden = q_in.shape[1]
    d_len = dm_ref.shape[1]
    dim = w_in.shape[1]
    block = pairs * q_len
    chips = group // CORES
    offsets = chip_offsets(chips)
    direct, relayed = slot_order(chips)
    tokens = group * block
    queries = group * pairs
    doc_rows = pairs * d_len
    tiles = doc_rows // ROWS
    depth = hidden // COLS

    me = lax.axis_index('data')
    chip = lax.div(me, CORES)
    core = lax.rem(me, CORES)
    partner = chip * CORES + (CORES - 1 - core)

    def at_offset(off):
        return lax.rem(chip + off + chips, chips)

    w_copy = pltpu.make_async_copy(w_hbm, w_in, w_sem)
    q_copy = pltpu.make_async_copy(q_hbm, q_in, q_sem)
    qm_copy = pltpu.make_async_copy(qm_hbm, qm_ref, qm_sem)
    dm_copy = pltpu.make_async_copy(dm_hbm, dm_ref, dm_sem)
    temp_copy = pltpu.make_async_copy(temp_hbm, temp_ref, temp_sem)

    def d_copy(i):
        rows = pl.ds(i * ROWS, ROWS)
        return pltpu.make_async_copy(d_hbm.at[rows], d_in.at[rows], d_sem.at[i])

    for copy in (w_copy, q_copy, qm_copy, dm_copy):
        copy.start()
    for i in range(EARLY):
        d_copy(i).start()
    temp_copy.start()

    barrier = pltpu.get_barrier_semaphore()
    for step in range(1, group):
        pl.semaphore_signal(barrier, inc=1, device_id={'data': lax.rem(me + step, group)}, device_id_type=MESH)

    def slot(s):
        return q_buf.at[pl.ds(s * block, block), :]

    def to_partner():
        return pltpu.make_async_remote_copy(slot(0), slot(1), q_send.at[0], q_recv.at[1],
                                            device_id={'data': partner}, device_id_type=MESH)

    def to_chip(k):
        back = offsets.index(-offsets[k]) if -offsets[k] in offsets else k
        place = direct[back]
        return pltpu.make_async_remote_copy(slot(0), slot(place), q_send.at[k], q_recv.at[place],
                                            device_id={'data': at_offset(offsets[k]) * CORES + core}, device_id_type=MESH)

    def relay(k):
        return pltpu.make_async_remote_copy(slot(direct[k]), slot(relayed[k]), relay_send.at[k], q_recv.at[relayed[k]],
                                            device_id={'data': partner}, device_id_type=MESH)

    def arrival(s):
        return pltpu.make_async_remote_copy(slot(s), slot(s), q_send.at[0], q_recv.at[s],
                                            device_id={'data': partner}, device_id_type=MESH)

    arrived = {0}

    def need(s):
        if s not in arrived:
            with jax.named_scope(f'need{s}'):
                arrival(s).wait_recv()
            arrived.add(s)

    def pass_on(k):
        need(direct[k])
        relay(k).start()

    score_tiles = tokens // COLS
    first_tile = [s * block // COLS for s in range(group)]
    ones = (lax.broadcasted_iota(jnp.int32, (COLS, dim), 1) == 0).astype(jnp.bfloat16)

    def project_queries():
        q_vecs = normalise(jnp.dot(q_in[...], w_in[...], preferred_element_type=jnp.float32))
        for t in range(q_len):
            keep = jnp.broadcast_to(qm_ref[:, t:t + 1], (pairs, dim)) == 1
            grid[t * pairs:(t + 1) * pairs, :] = jnp.where(keep, q_vecs[t * pairs:(t + 1) * pairs, :], 0.0)
        q_buf[0:block, :] = grid[0:block, :].astype(jnp.bfloat16)

    def project(doc):
        for first in range(doc * d_len, (doc + 1) * d_len, ROWS):
            raw = jnp.dot(d_in[first:first + ROWS, :], w_in[...], preferred_element_type=jnp.float32)
            part = first - doc * d_len
            masked = jnp.broadcast_to(dm_cols[part:part + ROWS, doc:doc + 1], (ROWS, dim))
            p_buf[first:first + ROWS, :] = jnp.where(masked == 0.0, normalise(raw), 0.0).astype(jnp.bfloat16)
            bias[first:first + ROWS, :] = masked.astype(jnp.bfloat16)

    def turn_masks():
        masked = jnp.where(dm_ref[...] == 1, 0.0, -BIG)
        masked = jnp.concatenate([masked, jnp.zeros((128 - pairs, d_len), jnp.float32)], axis=0)
        dm_cols[...] = jnp.transpose(masked)

    def score(n, docs):
        rhs = jnp.concatenate([q_buf[n * COLS:(n + 1) * COLS, :], ones], axis=1)
        for doc in docs:
            rows = slice(doc * d_len, (doc + 1) * d_len)
            lhs = jnp.concatenate([p_buf[rows, :], bias[rows, :]], axis=1)
            sim = lax.dot_general(lhs, rhs, (((1,), (1,)), ((), ())), preferred_element_type=jnp.float32)
            best[n % 2, doc:doc + 1, :] = jnp.max(sim, axis=0, keepdims=True)

    def send_later(turn):
        for k in range(1, chips):
            if SENDS[abs(offsets[k]) - 1] == turn:
                to_chip(k).start()

    def send_queries():
        with jax.named_scope('barrier'):
            pl.semaphore_wait(barrier, group - 1)
        to_partner().start()
        send_later(0)

    done = scored = 0
    with jax.named_scope('proj'):
        for step, count in enumerate(DOCS):
            if step == GREET_HIGH:
                pl.when(chip >= chips // 2)(send_queries)
            if step == GREET_LOW:
                pl.when(chip < chips // 2)(send_queries)
            for turn in range(1, max(SENDS) + 1):
                if step == GREET_HIGH + turn:
                    pl.when(chip >= chips // 2)(functools.partial(send_later, turn))
                if step == GREET_LOW + turn:
                    pl.when(chip < chips // 2)(functools.partial(send_later, turn))
            if step == HOME:
                need(1)
            if step == 0:
                with jax.named_scope('dmaw'):
                    w_copy.wait()
                    for i in range(EARLY, SOON):
                        d_copy(i).start()
                    q_copy.wait()
                    for i in range(SOON, ISSUED[0]):
                        d_copy(i).start()
                    qm_copy.wait()
                    dm_copy.wait()
                    if APART:
                        project_queries()
                        turn_masks()
            for i in range(ISSUED[step], ISSUED[step + 1]):
                d_copy(i).start()
            with jax.named_scope(f'dw{step}'):
                for i in range(done * d_len // ROWS, (done + count) * d_len // ROWS):
                    d_copy(i).wait()
            if step == 0 and not APART:
                project_queries()
                turn_masks()
            for doc in range(done, done + count):
                project(doc)
            if step >= HOME:
                score(0, range(scored, done))
                scored = done
            done += count

    sums = {}

    def fetch(n):
        after = min([f for f in FENCES if f > n] + [score_tiles])
        later = min([f for f in FENCES if f > after] + [score_tiles])
        for s in range(group):
            if first_tile[s] < after and s in direct:
                need(s)
        for k in range(1, chips):
            if first_tile[relayed[k]] < later and k not in passed:
                passed.add(k)
                pass_on(k)
        for s in range(group):
            if first_tile[s] < after:
                need(s)

    passed = set()

    def add_up(n):
        by_token = jnp.transpose(best[n % 2])
        for row in range(COLS // pairs):
            s = (n * COLS // pairs + row) // q_len
            term = by_token[row * pairs:(row + 1) * pairs, :]
            sums[s] = sums[s] + term if s in sums else term
        for s in [s for s in sums if (s + 1) * block <= (n + 1) * COLS]:
            place = direct if s in direct else relayed
            owner = at_offset(offsets[place.index(s)]) * CORES + (core if s in direct else CORES - 1 - core)
            grid[pl.ds(pl.multiple_of(owner * pairs, pairs), pairs), 0:pairs] = sums.pop(s)

    with jax.named_scope('scores'):
        for n in range(1, score_tiles):
            if n in FENCES:
                fetch(n)
            if n == 1:
                score(0, range(scored, pairs))
            score(n, range(pairs))
            add_up(n - 1)
        add_up(score_tiles - 1)
    scores = jnp.transpose(grid[0:queries, 0:pairs])

    with jax.named_scope('partial'):
        temp_copy.wait()
        z = scores / temp_ref[0]
        lane = lax.broadcasted_iota(jnp.int32, (pairs, queries), 1)
        sub = lax.broadcasted_iota(jnp.int32, (pairs, queries), 0)
        pos_grid = jnp.where(lane == me * pairs + sub, z, 0.0)
        pos_col = jnp.sum(pos_grid, axis=1, keepdims=True)
        pos_row = jnp.sum(pos_grid, axis=0, keepdims=True)
        col_max = jnp.max(z, axis=1, keepdims=True)
        lse_doc = jnp.log(jnp.sum(jnp.exp(z - col_max), axis=1, keepdims=True)) + col_max
        loss_doc = lse_doc - pos_col
        row_max = jnp.max(z, axis=0, keepdims=True)
        row_sum = jnp.sum(jnp.exp(z - row_max), axis=0, keepdims=True)
        doc_part = jnp.broadcast_to(jnp.sum(loss_doc - pos_col, axis=0, keepdims=True), (1, queries))
        fin[me] = jnp.concatenate([row_max, row_sum, doc_part, doc_part], axis=0)

    def share(step):
        to = lax.rem(me + step, group)
        return pltpu.make_async_remote_copy(fin.at[me], fin.at[me], fin_send.at[step - 1], fin_recv.at[step - 1],
                                            device_id={'data': to}, device_id_type=MESH)

    def shared(step):
        source = lax.rem(me - step + group, group)
        return pltpu.make_async_remote_copy(fin.at[source], fin.at[source], fin_send.at[step - 1], fin_recv.at[step - 1],
                                            device_id={'data': source}, device_id_type=MESH)

    for step in sorted(range(1, group), key=lambda step: abs(2 * step - group)):
        share(step).start()

    out_ref[1:2, 0:pairs] = jnp.sum(jnp.where(lane == sub, loss_doc, 0.0), axis=0, keepdims=True)[:, :pairs]

    with jax.named_scope('shwait'):
        to_partner().wait_send()
        for k in range(1, chips):
            to_chip(k).wait_send()
            relay(k).wait_send()
        for step in range(1, group):
            share(step).wait_send()
        for step in range(1, group):
            shared(step).wait_recv()

    with jax.named_scope('finish'):
        every = fin[...]
        maxes, sums = every[:, 0, :], every[:, 1, :]
        top = jnp.max(maxes, axis=0, keepdims=True)
        lse_query = jnp.log(jnp.sum(sums * jnp.exp(maxes - top), axis=0, keepdims=True)) + top
        loss_query = lse_query - pos_row
        own = jnp.where(lane == me * pairs + sub, loss_query, 0.0)
        own = jnp.sum(own, axis=1, keepdims=True)
        out_ref[0:1, 0:pairs] = jnp.sum(jnp.where(lane == sub, own, 0.0), axis=0, keepdims=True)[:, :pairs]
        total = jnp.sum(lse_query, axis=1, keepdims=True) + jnp.sum(every[:, 2, :], axis=0, keepdims=True)[:, :1]
        out_ref[2:3, 0:1] = total / (2 * queries)


def solution(mesh):
    group = mesh.shape['data']
    batch_spec = P(('replica', 'data'))

    def local_loss(q_hidden, d_hidden, w_proj, q_mask, d_mask, temperature):
        pairs, q_len, hidden = q_hidden.shape
        d_len = d_hidden.shape[1]
        dim = w_proj.shape[1]
        block = pairs * q_len
        chips = group // CORES
        vmem = pl.BlockSpec(memory_space=pltpu.VMEM)
        hbm = pl.BlockSpec(memory_space=pltpu.HBM)
        out = pl.pallas_call(
            functools.partial(kernel, group),
            out_shape=[jax.ShapeDtypeStruct((8, 128), jnp.float32)],
            in_specs=[hbm, hbm, hbm, hbm, hbm, hbm],
            out_specs=[vmem],
            scratch_shapes=[
                pltpu.SMEM((1,), jnp.float32),
                pltpu.VMEM((block, hidden), jnp.bfloat16),
                pltpu.VMEM((pairs * d_len, hidden), jnp.bfloat16),
                pltpu.VMEM((hidden, dim), jnp.bfloat16),
                pltpu.VMEM((pairs, q_len), jnp.int32),
                pltpu.VMEM((pairs, d_len), jnp.int32),
                pltpu.VMEM((group * block, dim), jnp.bfloat16),
                pltpu.VMEM((pairs * d_len, dim), jnp.bfloat16),
                pltpu.VMEM((pairs * d_len, dim), jnp.bfloat16),
                pltpu.VMEM((d_len, 128), jnp.float32),
                pltpu.VMEM((2, pairs, COLS), jnp.float32),
                pltpu.VMEM((max(block, group * pairs), dim), jnp.float32),
                pltpu.VMEM((group, 4, group * pairs), jnp.float32),
                pltpu.SemaphoreType.DMA,
                pltpu.SemaphoreType.DMA,
                pltpu.SemaphoreType.DMA,
                pltpu.SemaphoreType.DMA,
                pltpu.SemaphoreType.DMA,
                pltpu.SemaphoreType.DMA((pairs * d_len // ROWS,)),
                pltpu.SemaphoreType.DMA((chips,)),
                pltpu.SemaphoreType.DMA((group,)),
                pltpu.SemaphoreType.DMA((chips,)),
                pltpu.SemaphoreType.DMA((group - 1,)),
                pltpu.SemaphoreType.DMA((group - 1,)),
            ],
            compiler_params=pltpu.CompilerParams(collective_id=0, has_side_effects=True, vmem_limit_bytes=VMEM),
            name='late_interaction',
        )(temperature.reshape(1), q_hidden.transpose(1, 0, 2).reshape(block, hidden), d_hidden.reshape(pairs * d_len, hidden), w_proj, q_mask, d_mask)
        packed = out[0]
        def unpack(x_ref, q_ref, d_ref, m_ref):
            q_ref[...] = x_ref[0:1, 0:pairs]
            d_ref[...] = x_ref[1:2, 0:pairs]
            m_ref[...] = x_ref[2:3, 0:1]
        res = pl.pallas_call(unpack, out_shape=[jax.ShapeDtypeStruct((1, pairs), jnp.float32), jax.ShapeDtypeStruct((1, pairs), jnp.float32),
                       jax.ShapeDtypeStruct((1, 1), jnp.float32)], in_specs=[vmem], out_specs=[vmem, vmem, vmem],
                       compiler_params=pltpu.CompilerParams(vmem_limit_bytes=2 ** 20), name='unpack')(packed)
        return res[0].reshape(pairs), res[1].reshape(pairs), res[2].reshape(1)

    return jax.shard_map(local_loss, mesh=mesh, in_specs=(batch_spec, batch_spec, P(), batch_spec, batch_spec, P()),
                         out_specs=(batch_spec, batch_spec, P('replica')), check_vma=False)
```
